32 devices in a mesh: blk: 16 (over z, y, x), rep: 2 (over core).
Axes of the slice: x: 2, y: 2, z: 4, core: 2. Of those that a mesh axis runs over, the one named last changes fastest.
Arguments:
- points: float32 [16, 3, 8192], P('blk'), may hold values from -6 to 6
- normals: float32 [16, 3, 8192], P('blk'), may hold values from -6 to 6
- src_block: int32 [8, 16, 1, 16], P(None, 'blk', None, 'rep'), may hold values from 0 to 63
- tgt_index: int32 [8, 16, 1, 16, 128], P(None, 'blk', None, 'rep'), may hold values from 0 to 8191
- active: int32 [8, 16, 1], P(None, 'blk'), may hold values from 0 to 16
Outputs:
- diag_hess: float32 [16, 36], P('blk')
- gradient: float32 [16, 6], P('blk')
- pair_hess: float32 [8, 16, 1, 36], P(None, 'blk')
The draws below stay inside these ranges and needn't reach their ends.
Inputs may be any that keep to these rules, and one draw needn't show every extreme that they name: Slots j with j >= active contribute nothing.
All inputs are finite; a program needn't handle non-finite values.
Results may differ from the reference program's by a relative error of at most 0.00017.
Values sent between devices are 32-bit elements; how exact they have to be, the bound alone decides.
A program may use at most 64 MiB of HBM per device.

```python
import jax
import jax.numpy as jnp
from jax import lax

SC = 1
P_SIZE = 8192
NB = 16
BLOCK = 128
ROUNDS = 8
NSCANS = 16
N_BLK = 16


def place_ends(values, key, low, high):
    longest = values.shape.index(max(values.shape))
    spots = []
    for shift in (0, 1):
        where = [jax.random.randint(jax.random.fold_in(key, axis), (), 0, length) for axis, length in enumerate(values.shape)]
        where[longest] = (where[longest] + shift) % values.shape[longest]
        spots.append(tuple(where))
    return values.at[spots[0]].set(low).at[spots[1]].set(high)


def level_of(rng, extent, shards, low, high):
    level = 1.0
    for dim, shards_of in shards:
        steps = jax.random.uniform(jax.random.fold_in(jax.random.fold_in(rng, 6), dim), (shards_of,), jnp.float32, low / len(shards), high / len(shards))
        level = level * jnp.repeat(jnp.exp(steps), extent[dim] // shards_of).reshape((-1,) + (1,) * (len(extent) - 1 - dim))
    return level


def gaussian(key, extent, width, limit, pieces=(), kind=jnp.bfloat16):
    gain = level_of(key, extent, pieces, -0.22, 0.18) if pieces else 1.0
    drawn = jax.random.normal(key, extent, jnp.float32) * width * gain
    return jnp.minimum(jnp.maximum(drawn, -limit), limit).astype(kind)


def setup_inputs(seed: int = 0) -> dict:
    key_of = jax.random.split(jax.random.key(seed), 6)
    return {
        "points": gaussian(key_of[0], (NSCANS, 3, P_SIZE), 0.5, 6.0, ((0, 16),), jnp.float32),
        "normals": gaussian(key_of[1], (NSCANS, 3, P_SIZE), 1.0, 6.0, ((0, 16),), jnp.float32),
        "src_block": place_ends(jax.random.randint(key_of[2], (ROUNDS, NSCANS, SC, NB), 0, P_SIZE // BLOCK), jax.random.fold_in(key_of[2], 1), 0, (P_SIZE // BLOCK) - 1).astype(jnp.int32),
        "tgt_index": place_ends(jax.random.randint(key_of[3], (ROUNDS, NSCANS, SC, NB, BLOCK), 0, P_SIZE), jax.random.fold_in(key_of[3], 1), 0, P_SIZE - 1).astype(jnp.int32),
        "active": place_ends(jax.random.randint(key_of[4], (ROUNDS, NSCANS, SC), 0, NB + 1), jax.random.fold_in(key_of[4], 1), 0, NB).astype(jnp.int32),
    }


def reference(points, normals, src_block, tgt_index, active):
    nscans = points.shape[0]
    npts = points.shape[2]
    slots = NB * BLOCK
    flat_p = jnp.moveaxis(points, 1, 0).reshape(3, -1)
    flat_n = jnp.moveaxis(normals, 1, 0).reshape(3, -1)
    lanes = jnp.arange(BLOCK, dtype=jnp.int32)
    owner = jnp.arange(nscans, dtype=jnp.int32) // SC
    local = jnp.arange(SC, dtype=jnp.int32)
    scans = jnp.arange(nscans, dtype=jnp.int32)
    slot_block = jnp.arange(slots, dtype=jnp.int32) // BLOCK
    diag = jnp.zeros((nscans, 36), jnp.float32)
    grad = jnp.zeros((nscans, 6), jnp.float32)
    pairs = []
    for k in range(1, ROUNDS + 1):
        tscan = (((owner[:, None] - k) % N_BLK) * SC + local[None, :]).astype(jnp.int32)
        sidx = (scans[:, None, None, None] * npts + src_block[k - 1][:, :, :, None] * BLOCK + lanes).reshape(nscans, SC, slots)
        tidx = tscan[:, :, None] * npts + tgt_index[k - 1].reshape(nscans, SC, slots)
        p = flat_p[:, sidx]
        q = flat_p[:, tidx]
        n = flat_n[:, tidx]
        live = (slot_block[None, None, :] < active[k - 1][:, :, None]).astype(jnp.float32)
        resid = jnp.sum(n * (p - q), axis=0)
        weight = live / (1.0 + resid * resid)
        jacob = jnp.stack([p[1] * n[2] - p[2] * n[1], p[2] * n[0] - p[0] * n[2], p[0] * n[1] - p[1] * n[0], n[0], n[1], n[2]])
        gram = jnp.einsum('iast,jast->asij', jacob * weight, jacob, precision=lax.Precision.HIGHEST) / (NB * BLOCK)
        push = jnp.einsum('iast,ast->asi', jacob, weight * resid, precision=lax.Precision.HIGHEST) / (NB * BLOCK)
        gram = gram.reshape(nscans, SC, 36)
        pairs.append(gram)
        diag = diag + gram.sum(1)
        grad = grad + push.sum(1)
        diag = diag.at[tscan.reshape(-1)].add(gram.reshape(-1, 36))
        grad = grad.at[tscan.reshape(-1)].add(-push.reshape(-1, 6))
    scale = 2.0 * ROUNDS * SC
    return diag / scale, grad / scale, jnp.stack(pairs)
```

```python
import functools

import jax
import jax.numpy as jnp
from jax import lax
from jax.experimental import pallas as pl
from jax.experimental.pallas import tpu as pltpu
from jax.sharding import PartitionSpec as P

BLOCK = 128
MESH = pl.DeviceIdType.MESH


def kernel(
    n, reps, pts, nrm, src, tgt, act, diag_ref, grad_ref, pair_ref,
    stage, inbox, prod, res, got, own, other,
    out_send, out_recv, back_send, back_recv, pair_send, pair_recv,
):
    rounds, per_rep = tgt.shape[0], tgt.shape[3]
    npts = pts.shape[1] * BLOCK
    me = lax.axis_index("blk")
    half = lax.axis_index("rep")
    partner = 1 - half

    offsets = sorted({k % n for k in range(1, rounds + 1)} | {-k % n for k in range(1, rounds + 1)})
    barrier = pltpu.get_barrier_semaphore()
    for d in offsets:
        for r in range(reps):
            pl.semaphore_signal(
                barrier, inc=1, device_id={"blk": lax.rem(me + d, n), "rep": r}, device_id_type=MESH
            )
    pl.semaphore_signal(barrier, inc=1, device_id={"blk": me, "rep": partner}, device_id_type=MESH)

    slot = lax.broadcasted_iota(jnp.int32, (per_rep, BLOCK), 0) + half * per_rep
    for k in range(rounds):
        for j in range(per_rep):
            block = src[k, 0, 0, j]
            for c in range(3):
                stage[k, c * per_rep + j, :] = pts[c, block]
        index = jnp.where(slot < act[0, k], tgt[k, 0, 0], npts)
        stage[k, 3 * per_rep :, :] = index.astype(jnp.float32)
    prod[...] = jnp.zeros_like(prod)
    res[...] = jnp.zeros_like(res)

    pl.semaphore_wait(barrier, len(offsets) * reps + 1)

    def outgoing(k):
        return pltpu.make_async_remote_copy(
            src_ref=stage.at[k],
            dst_ref=inbox.at[k],
            send_sem=out_send.at[k],
            recv_sem=out_recv.at[k],
            device_id={"blk": lax.rem(me + n - (k + 1), n), "rep": half},
            device_id_type=MESH,
        )

    def returned(k, r):
        return pltpu.make_async_remote_copy(
            src_ref=res.at[k],
            dst_ref=got.at[k, half],
            send_sem=back_send.at[k, r],
            recv_sem=back_recv.at[k, half],
            device_id={"blk": lax.rem(me + k + 1, n), "rep": r},
            device_id_type=MESH,
        )

    def arrival(k, r):
        return pltpu.make_async_remote_copy(
            src_ref=res.at[k],
            dst_ref=got.at[k, r],
            send_sem=back_send.at[k, r],
            recv_sem=back_recv.at[k, r],
            device_id={"blk": lax.rem(me + k + 1, n), "rep": r},
            device_id_type=MESH,
        )

    for k in range(rounds):
        outgoing(k).start()

    def one_round(k, carry):
        outgoing(k).wait_recv()
        p = [inbox[k, c * per_rep : (c + 1) * per_rep, :] for c in range(3)]
        index = inbox[k, 3 * per_rep :, :].astype(jnp.int32)
        lane = index & (BLOCK - 1)
        row = index >> (BLOCK.bit_length() - 1)
        found = [jnp.zeros((per_rep, BLOCK), jnp.float32) for _ in range(6)]
        for h in range(npts // BLOCK):
            here = row == h
            for c in range(6):
                table = pts if c < 3 else nrm
                line = table[c % 3, h : h + 1, :]
                line = jnp.broadcast_to(line, (per_rep, BLOCK))
                value = jnp.take_along_axis(line, lane, axis=1, mode="promise_in_bounds")
                found[c] = jnp.where(here, value, found[c])
        q, m = found[:3], found[3:]
        resid = m[0] * (p[0] - q[0]) + m[1] * (p[1] - q[1]) + m[2] * (p[2] - q[2])
        weight = 1.0 / (1.0 + resid * resid)
        jacob = [
            p[1] * m[2] - p[2] * m[1],
            p[2] * m[0] - p[0] * m[2],
            p[0] * m[1] - p[1] * m[0],
            m[0],
            m[1],
            m[2],
        ]
        for i in range(6):
            scaled = jacob[i] * weight
            for j in range(i, 6):
                line = jnp.sum(scaled * jacob[j], axis=0, keepdims=True)
                prod[k, 6 * i + j : 6 * i + j + 1, :] = line
                if j != i:
                    prod[k, 6 * j + i : 6 * j + i + 1, :] = line
            prod[k, 36 + i : 37 + i, :] = jnp.sum(scaled * resid, axis=0, keepdims=True)
        return carry

    lax.fori_loop(0, rounds, one_round, 0)

    width = prod.shape[1]
    ones = jnp.ones((8, BLOCK), jnp.float32)
    for k in range(rounds):
        sums = lax.dot_general(
            ones, prod[k], (((1,), (1,)), ((), ())),
            precision=lax.Precision.HIGHEST, preferred_element_type=jnp.float32,
        )
        res[k, :, :width] = sums[:1] / (reps * per_rep * BLOCK)
    for k in range(rounds):
        for r in range(reps):
            returned(k, r).start()
    lanes = lax.broadcasted_iota(jnp.int32, (1, BLOCK), 1)
    sign = jnp.where(lanes < 36, 1.0, -1.0)
    total = res[0]
    for k in range(1, rounds):
        total = total + res[k]
    own[...] = total * sign
    swap = pltpu.make_async_remote_copy(
        src_ref=own,
        dst_ref=other,
        send_sem=pair_send,
        recv_sem=pair_recv,
        device_id={"blk": me, "rep": partner},
        device_id_type=MESH,
    )
    swap.start()
    for k in range(rounds):
        outgoing(k).wait_send()
    swap.wait()
    total = own[...] + other[...]
    for k in range(rounds):
        for r in range(reps):
            arrival(k, r).wait_recv()
        both = got[k, 0] + got[k, 1]
        pair_ref[k, 0] = both[:, :36]
        total = total + both
    scale = 2.0 * rounds
    total = total / scale
    diag_ref[...] = total[:, :36]
    grad_ref[...] = total[:, 36:42]
    for k in range(rounds):
        for r in range(reps):
            returned(k, r).wait_send()


def by_rows(scan):
    return jnp.moveaxis(scan, 1, 0).reshape(scan.shape[1], -1, BLOCK)


def body(n, reps, points, normals, src_block, tgt_index, active):
    rounds, count = src_block.shape[:2]
    per_rep = src_block.shape[3]
    if count != 1 or reps != 2 or rounds >= n:
        raise ValueError("unsupported sizes")
    vmem = pl.BlockSpec(memory_space=pltpu.VMEM)
    smem = pl.BlockSpec(memory_space=pltpu.SMEM)
    f32 = jnp.float32
    return pl.pallas_call(
        functools.partial(kernel, n, reps),
        out_shape=(
            jax.ShapeDtypeStruct((1, 36), f32),
            jax.ShapeDtypeStruct((1, 6), f32),
            jax.ShapeDtypeStruct((rounds, 1, 1, 36), f32),
        ),
        in_specs=[vmem, vmem, smem, vmem, smem],
        out_specs=(vmem, vmem, vmem),
        scratch_shapes=[
            pltpu.VMEM((rounds, 4 * per_rep, BLOCK), f32),
            pltpu.VMEM((rounds, 4 * per_rep, BLOCK), f32),
            pltpu.VMEM((rounds, 48, BLOCK), f32),
            pltpu.VMEM((rounds, 1, BLOCK), f32),
            pltpu.VMEM((rounds, reps, 1, BLOCK), f32),
            pltpu.VMEM((1, BLOCK), f32),
            pltpu.VMEM((1, BLOCK), f32),
            pltpu.SemaphoreType.DMA((rounds,)),
            pltpu.SemaphoreType.DMA((rounds,)),
            pltpu.SemaphoreType.DMA((rounds, reps)),
            pltpu.SemaphoreType.DMA((rounds, reps)),
            pltpu.SemaphoreType.DMA,
            pltpu.SemaphoreType.DMA,
        ],
        compiler_params=pltpu.CompilerParams(collective_id=0, has_side_effects=True),
        name="normal_equations",
    )(by_rows(points), by_rows(normals), src_block, tgt_index, active.reshape(1, rounds))


def solution(mesh):
    return jax.shard_map(
        functools.partial(body, mesh.shape["blk"], mesh.shape["rep"]),
        mesh=mesh,
        in_specs=(
            P("blk", None, None),
            P("blk", None, None),
            P(None, "blk", None, "rep"),
            P(None, "blk", None, "rep", None),
            P(None, "blk", None),
        ),
        out_specs=(P("blk", None), P("blk", None), P(None, "blk", None, None)),
        check_vma=False,
    )
```

```python
import functools

import jax
import jax.numpy as jnp
from jax import lax
from jax.experimental import pallas as pl
from jax.experimental.pallas import tpu as pltpu
from jax.sharding import PartitionSpec as P

BLOCK = 128
MESH = pl.DeviceIdType.MESH


def schedule(rounds):
    bits = sorted(range(1, rounds + 1), key=lambda k: (k.bit_count(), k))
    near = [k for k in bits if k.bit_count() == 1]
    return [k - 1 for k in near[1:2] + near[3:] + near[:1] + bits[len(near) :] + near[2:3]]


def kernel(
    n, reps, pts_hbm, nrm_hbm, src_hbm, tgt_hbm, act_hbm, out,
    pts, nrm, src, tgt, act, stage, inbox, prod, res, got, own, other,
    load, out_send, out_recv, back_send, back_recv, pair_send, pair_recv,
):
    rounds, per_rep = tgt.shape[0], tgt.shape[3]
    npts = pts.shape[1] * BLOCK
    me = lax.axis_index("blk")
    half = lax.axis_index("rep")
    partner = 1 - half
    order = schedule(rounds)

    offsets = sorted({k % n for k in range(1, rounds + 1)} | {-k % n for k in range(1, rounds + 1)})
    barrier = pltpu.get_barrier_semaphore()
    for d in offsets:
        for r in range(reps):
            pl.semaphore_signal(
                barrier, inc=1, device_id={"blk": lax.rem(me + d, n), "rep": r}, device_id_type=MESH
            )
    pl.semaphore_signal(barrier, inc=1, device_id={"blk": me, "rep": partner}, device_id_type=MESH)

    pairs = ((src_hbm, src), (act_hbm, act), (tgt_hbm, tgt), (pts_hbm, pts), (nrm_hbm, nrm))
    loads = [pltpu.make_async_copy(a, b, load.at[i]) for i, (a, b) in enumerate(pairs)]
    for copy in loads:
        copy.start()
    prod[...] = jnp.zeros_like(prod)
    res[...] = jnp.zeros_like(res)
    for copy in loads[:4]:
        copy.wait()

    slot = lax.broadcasted_iota(jnp.int32, (per_rep, BLOCK), 0) + half * per_rep
    for k in range(rounds):
        for j in range(per_rep):
            block = src[k, 0, 0, j]
            for c in range(3):
                stage[k, c * per_rep + j, :] = pts[c, block]
        index = jnp.where(slot < act[0, k], tgt[k, 0, 0], npts)
        stage[k, 3 * per_rep :, :] = index.astype(jnp.float32)

    pl.semaphore_wait(barrier, len(offsets) * reps + 1)

    def outgoing(k):
        return pltpu.make_async_remote_copy(
            src_ref=stage.at[k],
            dst_ref=inbox.at[k],
            send_sem=out_send.at[k],
            recv_sem=out_recv.at[k],
            device_id={"blk": lax.rem(me + n - (k + 1), n), "rep": half},
            device_id_type=MESH,
        )

    def returned(k, r):
        return pltpu.make_async_remote_copy(
            src_ref=res.at[k],
            dst_ref=got.at[k, half],
            send_sem=back_send.at[k, r],
            recv_sem=back_recv.at[k, half],
            device_id={"blk": lax.rem(me + k + 1, n), "rep": r},
            device_id_type=MESH,
        )

    def arrival(k, r):
        return pltpu.make_async_remote_copy(
            src_ref=res.at[k],
            dst_ref=got.at[k, r],
            send_sem=back_send.at[k, r],
            recv_sem=back_recv.at[k, r],
            device_id={"blk": lax.rem(me + k + 1, n), "rep": r},
            device_id_type=MESH,
        )

    for k in order:
        outgoing(k).start()
    loads[4].wait()

    def terms(k):
        p = [inbox[k, c * per_rep : (c + 1) * per_rep, :] for c in range(3)]
        index = inbox[k, 3 * per_rep :, :].astype(jnp.int32)
        lane = index & (BLOCK - 1)
        row = index >> (BLOCK.bit_length() - 1)
        found = [jnp.zeros((per_rep, BLOCK), jnp.float32) for _ in range(6)]
        for h in range(npts // BLOCK):
            here = row == h
            for c in range(6):
                table = pts if c < 3 else nrm
                line = table[c % 3, h : h + 1, :]
                line = jnp.broadcast_to(line, (per_rep, BLOCK))
                value = jnp.take_along_axis(line, lane, axis=1, mode="promise_in_bounds")
                found[c] = jnp.where(here, value, found[c])
        q, m = found[:3], found[3:]
        resid = m[0] * (p[0] - q[0]) + m[1] * (p[1] - q[1]) + m[2] * (p[2] - q[2])
        weight = 1.0 / (1.0 + resid * resid)
        jacob = [
            p[1] * m[2] - p[2] * m[1],
            p[2] * m[0] - p[0] * m[2],
            p[0] * m[1] - p[1] * m[0],
            m[0],
            m[1],
            m[2],
        ]
        for i in range(6):
            scaled = jacob[i] * weight
            for j in range(i, 6):
                line = jnp.sum(scaled * jacob[j], axis=0, keepdims=True)
                prod[k, 6 * i + j : 6 * i + j + 1, :] = line
                if j != i:
                    prod[k, 6 * j + i : 6 * j + i + 1, :] = line
            prod[k, 36 + i : 37 + i, :] = jnp.sum(scaled * resid, axis=0, keepdims=True)

    width = prod.shape[1]
    ones = jnp.ones((8, BLOCK), jnp.float32)

    def lane_sums(k):
        sums = lax.dot_general(
            ones, prod[k], (((1,), (1,)), ((), ())),
            precision=lax.Precision.HIGHEST, preferred_element_type=jnp.float32,
        )
        res[k, :, :width] = sums[:1] / (reps * per_rep * BLOCK)

    before = None
    for k in order:
        outgoing(k).wait_recv()
        if before is not None:
            lane_sums(before)
        terms(k)
        if before is not None:
            for r in range(reps):
                returned(before, r).start()
        before = k
    lane_sums(before)
    for r in range(reps):
        returned(before, r).start()
    lanes = lax.broadcasted_iota(jnp.int32, (1, BLOCK), 1)
    sign = jnp.where(lanes < 36, 1.0, -1.0)
    total = res[0]
    for k in range(1, rounds):
        total = total + res[k]
    own[...] = total * sign
    swap = pltpu.make_async_remote_copy(
        src_ref=own,
        dst_ref=other,
        send_sem=pair_send,
        recv_sem=pair_recv,
        device_id={"blk": me, "rep": partner},
        device_id_type=MESH,
    )
    swap.start()
    for k in order:
        outgoing(k).wait_send()
    swap.wait()
    total = own[...] + other[...]
    for k in order:
        for r in range(reps):
            arrival(k, r).wait_recv()
        both = got[k, 0] + got[k, 1]
        out[k : k + 1, :] = both
        total = total + both
    out[rounds : rounds + 1, :] = total / (2.0 * rounds)
    for k in order:
        for r in range(reps):
            returned(k, r).wait_send()


def split(sums, diag_ref, grad_ref, pair_ref):
    rounds = pair_ref.shape[0]
    for k in range(rounds):
        pair_ref[k, 0] = sums[k : k + 1, :36]
    diag_ref[...] = sums[rounds : rounds + 1, :36]
    grad_ref[...] = sums[rounds : rounds + 1, 36:42]


def by_rows(scan):
    return jnp.moveaxis(scan, 1, 0).reshape(scan.shape[1], -1, BLOCK)


def body(n, reps, points, normals, src_block, tgt_index, active):
    rounds, count = src_block.shape[:2]
    per_rep = src_block.shape[3]
    if count != 1 or reps != 2 or rounds >= n:
        raise ValueError("unsupported sizes")
    vmem = pl.BlockSpec(memory_space=pltpu.VMEM)
    f32, i32 = jnp.float32, jnp.int32
    rows = points.shape[2] // BLOCK
    sums = pl.pallas_call(
        functools.partial(kernel, n, reps),
        out_shape=jax.ShapeDtypeStruct((rounds + 1, BLOCK), f32),
        in_specs=[pl.BlockSpec(memory_space=pl.ANY)] * 5,
        out_specs=vmem,
        scratch_shapes=[
            pltpu.VMEM((3, rows, BLOCK), f32),
            pltpu.VMEM((3, rows, BLOCK), f32),
            pltpu.SMEM(src_block.shape, i32),
            pltpu.VMEM(tgt_index.shape, i32),
            pltpu.SMEM((1, rounds), i32),
            pltpu.VMEM((rounds, 4 * per_rep, BLOCK), f32),
            pltpu.VMEM((rounds, 4 * per_rep, BLOCK), f32),
            pltpu.VMEM((rounds, 48, BLOCK), f32),
            pltpu.VMEM((rounds, 1, BLOCK), f32),
            pltpu.VMEM((rounds, reps, 1, BLOCK), f32),
            pltpu.VMEM((1, BLOCK), f32),
            pltpu.VMEM((1, BLOCK), f32),
            pltpu.SemaphoreType.DMA((5,)),
            pltpu.SemaphoreType.DMA((rounds,)),
            pltpu.SemaphoreType.DMA((rounds,)),
            pltpu.SemaphoreType.DMA((rounds, reps)),
            pltpu.SemaphoreType.DMA((rounds, reps)),
            pltpu.SemaphoreType.DMA,
            pltpu.SemaphoreType.DMA,
        ],
        compiler_params=pltpu.CompilerParams(collective_id=0, has_side_effects=True),
        name="normal_equations",
    )(by_rows(points), by_rows(normals), src_block, tgt_index, active.reshape(1, rounds))
    return pl.pallas_call(
        split,
        out_shape=(
            jax.ShapeDtypeStruct((1, 36), f32),
            jax.ShapeDtypeStruct((1, 6), f32),
            jax.ShapeDtypeStruct((rounds, 1, 1, 36), f32),
        ),
        in_specs=[vmem],
        out_specs=(vmem, vmem, vmem),
        name="split_sums",
    )(sums)


def solution(mesh):
    return jax.shard_map(
        functools.partial(body, mesh.shape["blk"], mesh.shape["rep"]),
        mesh=mesh,
        in_specs=(
            P("blk", None, None),
            P("blk", None, None),
            P(None, "blk", None, "rep"),
            P(None, "blk", None, "rep", None),
            P(None, "blk", None),
        ),
        out_specs=(P("blk", None), P("blk", None), P(None, "blk", None, None)),
        check_vma=False,
    )
```

```python
import functools

import jax
import jax.numpy as jnp
from jax import lax
from jax.experimental import pallas as pl
from jax.experimental.pallas import tpu as pltpu
from jax.sharding import PartitionSpec as P

BLOCK = 128
MESH = pl.DeviceIdType.MESH


def schedule(rounds):
    bits = sorted(range(1, rounds + 1), key=lambda k: (k.bit_count(), k))
    near = [k for k in bits if k.bit_count() == 1]
    return [k - 1 for k in near[1:2] + near[3:] + near[:1] + bits[len(near) :] + near[2:3]]


def kernel(
    n, reps, pts_hbm, nrm_hbm, src_hbm, tgt_hbm, act_hbm, out,
    pts, nrm, src, tgt, act, stage, inbox, prod, res, got, own, other,
    load, out_send, out_recv, back_send, back_recv, pair_send, pair_recv,
):
    rounds, per_rep = tgt.shape[0], tgt.shape[3]
    npts = pts.shape[1] * BLOCK
    me = lax.axis_index("blk")
    half = lax.axis_index("rep")
    partner = 1 - half
    order = schedule(rounds)

    offsets = sorted({k % n for k in range(1, rounds + 1)} | {-k % n for k in range(1, rounds + 1)})
    barrier = pltpu.get_barrier_semaphore()
    for d in offsets:
        for r in range(reps):
            pl.semaphore_signal(
                barrier, inc=1, device_id={"blk": lax.rem(me + d, n), "rep": r}, device_id_type=MESH
            )
    pl.semaphore_signal(barrier, inc=1, device_id={"blk": me, "rep": partner}, device_id_type=MESH)

    pairs = ((src_hbm, src), (act_hbm, act), (tgt_hbm, tgt), (pts_hbm, pts), (nrm_hbm, nrm))
    loads = [pltpu.make_async_copy(a, b, load.at[i]) for i, (a, b) in enumerate(pairs)]
    for copy in loads:
        copy.start()
    prod[...] = jnp.zeros_like(prod)
    res[...] = jnp.zeros_like(res)
    for copy in loads[:4]:
        copy.wait()

    slot = lax.broadcasted_iota(jnp.int32, (per_rep, BLOCK), 0) + half * per_rep
    for k in range(rounds):
        for j in range(per_rep):
            block = src[k, 0, 0, j]
            for c in range(3):
                stage[k, c * per_rep + j, :] = pts[c, block]
        index = jnp.where(slot < act[0, k], tgt[k, 0, 0], npts)
        stage[k, 3 * per_rep :, :] = index.astype(jnp.float32)

    pl.semaphore_wait(barrier, len(offsets) * reps + 1)

    def outgoing(k):
        return pltpu.make_async_remote_copy(
            src_ref=stage.at[k],
            dst_ref=inbox.at[k],
            send_sem=out_send.at[k],
            recv_sem=out_recv.at[k],
            device_id={"blk": lax.rem(me + n - (k + 1), n), "rep": half},
            device_id_type=MESH,
        )

    def returned(k, r):
        return pltpu.make_async_remote_copy(
            src_ref=res.at[k],
            dst_ref=got.at[k, half],
            send_sem=back_send.at[k, r],
            recv_sem=back_recv.at[k, half],
            device_id={"blk": lax.rem(me + k + 1, n), "rep": r},
            device_id_type=MESH,
        )

    def arrival(k, r):
        return pltpu.make_async_remote_copy(
            src_ref=res.at[k],
            dst_ref=got.at[k, r],
            send_sem=back_send.at[k, r],
            recv_sem=back_recv.at[k, r],
            device_id={"blk": lax.rem(me + k + 1, n), "rep": r},
            device_id_type=MESH,
        )

    for k in order:
        outgoing(k).start()
    loads[4].wait()

    def terms(k):
        p = [inbox[k, c * per_rep : (c + 1) * per_rep, :] for c in range(3)]
        index = inbox[k, 3 * per_rep :, :].astype(jnp.int32)
        lane = index & (BLOCK - 1)
        row = index >> (BLOCK.bit_length() - 1)
        found = [jnp.zeros((per_rep, BLOCK), jnp.float32) for _ in range(6)]
        for h in range(npts // BLOCK):
            here = row == h
            for c in range(6):
                table = pts if c < 3 else nrm
                line = table[c % 3, h : h + 1, :]
                line = jnp.broadcast_to(line, (per_rep, BLOCK))
                value = jnp.take_along_axis(line, lane, axis=1, mode="promise_in_bounds")
                found[c] = jnp.where(here, value, found[c])
        q, m = found[:3], found[3:]
        resid = m[0] * (p[0] - q[0]) + m[1] * (p[1] - q[1]) + m[2] * (p[2] - q[2])
        weight = 1.0 / (1.0 + resid * resid)
        jacob = [
            p[1] * m[2] - p[2] * m[1],
            p[2] * m[0] - p[0] * m[2],
            p[0] * m[1] - p[1] * m[0],
            m[0],
            m[1],
            m[2],
        ]
        for i in range(6):
            scaled = jacob[i] * weight
            for j in range(i, 6):
                line = jnp.sum(scaled * jacob[j], axis=0, keepdims=True)
                prod[k, 6 * i + j : 6 * i + j + 1, :] = line
                if j != i:
                    prod[k, 6 * j + i : 6 * j + i + 1, :] = line
            prod[k, 36 + i : 37 + i, :] = jnp.sum(scaled * resid, axis=0, keepdims=True)

    width = prod.shape[1]
    ones = jnp.ones((8, BLOCK), jnp.float32)

    def lane_sums(k):
        sums = lax.dot_general(
            ones, prod[k], (((1,), (1,)), ((), ())),
            precision=lax.Precision.HIGHEST, preferred_element_type=jnp.float32,
        )
        res[k, :, :width] = sums[:1] / (reps * per_rep * BLOCK)

    before = None
    for k in order:
        outgoing(k).wait_recv()
        if before is not None:
            lane_sums(before)
        terms(k)
        if before is not None:
            for r in range(reps):
                returned(before, r).start()
        before = k
    lane_sums(before)
    for r in range(reps):
        returned(before, r).start()
    lanes = lax.broadcasted_iota(jnp.int32, (1, BLOCK), 1)
    sign = jnp.where(lanes < 36, 1.0, -1.0)
    total = res[0]
    for k in range(1, rounds):
        total = total + res[k]
    own[...] = total * sign
    swap = pltpu.make_async_remote_copy(
        src_ref=own,
        dst_ref=other,
        send_sem=pair_send,
        recv_sem=pair_recv,
        device_id={"blk": me, "rep": partner},
        device_id_type=MESH,
    )
    swap.start()
    for k in order:
        outgoing(k).wait_send()
    swap.wait()
    total = own[...] + other[...]
    for k in order:
        for r in range(reps):
            arrival(k, r).wait_recv()
        both = got[k, 0] + got[k, 1]
        out[k : k + 1, :] = both
        total = total + both
    out[rounds : rounds + 1, :] = total / (2.0 * rounds)
    for k in order:
        for r in range(reps):
            returned(k, r).wait_send()


def split(sums, diag_ref, grad_ref, pair_ref):
    rounds = pair_ref.shape[0]
    for k in range(rounds):
        pair_ref[k, 0] = sums[k : k + 1, :36]
    diag_ref[...] = sums[rounds : rounds + 1, :36]
    grad_ref[...] = sums[rounds : rounds + 1, 36:42]


def by_rows(scan):
    return jnp.moveaxis(scan, 1, 0).reshape(scan.shape[1], -1, BLOCK)


def body(n, reps, points, normals, src_block, tgt_index, active):
    rounds, count = src_block.shape[:2]
    per_rep = src_block.shape[3]
    if count != 1 or reps != 2 or rounds >= n:
        raise ValueError("unsupported sizes")
    vmem = pl.BlockSpec(memory_space=pltpu.VMEM)
    f32, i32 = jnp.float32, jnp.int32
    rows = points.shape[2] // BLOCK
    sums = pl.pallas_call(
        functools.partial(kernel, n, reps),
        out_shape=pltpu.VMEM((rounds + 1, BLOCK), f32),
        in_specs=[pl.BlockSpec(memory_space=pl.ANY)] * 5,
        out_specs=vmem,
        scratch_shapes=[
            pltpu.VMEM((3, rows, BLOCK), f32),
            pltpu.VMEM((3, rows, BLOCK), f32),
            pltpu.SMEM(src_block.shape, i32),
            pltpu.VMEM(tgt_index.shape, i32),
            pltpu.SMEM((1, rounds), i32),
            pltpu.VMEM((rounds, 4 * per_rep, BLOCK), f32),
            pltpu.VMEM((rounds, 4 * per_rep, BLOCK), f32),
            pltpu.VMEM((rounds, 48, BLOCK), f32),
            pltpu.VMEM((rounds, 1, BLOCK), f32),
            pltpu.VMEM((rounds, reps, 1, BLOCK), f32),
            pltpu.VMEM((1, BLOCK), f32),
            pltpu.VMEM((1, BLOCK), f32),
            pltpu.SemaphoreType.DMA((5,)),
            pltpu.SemaphoreType.DMA((rounds,)),
            pltpu.SemaphoreType.DMA((rounds,)),
            pltpu.SemaphoreType.DMA((rounds, reps)),
            pltpu.SemaphoreType.DMA((rounds, reps)),
            pltpu.SemaphoreType.DMA,
            pltpu.SemaphoreType.DMA,
        ],
        compiler_params=pltpu.CompilerParams(collective_id=0, has_side_effects=True),
        name="normal_equations",
    )(by_rows(points), by_rows(normals), src_block, tgt_index, active.reshape(1, rounds))
    return pl.pallas_call(
        split,
        out_shape=(
            jax.ShapeDtypeStruct((1, 36), f32),
            jax.ShapeDtypeStruct((1, 6), f32),
            jax.ShapeDtypeStruct((rounds, 1, 1, 36), f32),
        ),
        in_specs=[vmem],
        out_specs=(vmem, vmem, vmem),
        name="split_sums",
    )(pltpu.with_memory_space_constraint(sums, pltpu.VMEM))


def solution(mesh):
    return jax.shard_map(
        functools.partial(body, mesh.shape["blk"], mesh.shape["rep"]),
        mesh=mesh,
        in_specs=(
            P("blk", None, None),
            P("blk", None, None),
            P(None, "blk", None, "rep"),
            P(None, "blk", None, "rep", None),
            P(None, "blk", None),
        ),
        out_specs=(P("blk", None), P("blk", None), P(None, "blk", None, None)),
        check_vma=False,
    )
```

```python
import functools

import jax
import jax.numpy as jnp
from jax import lax
from jax.experimental import pallas as pl
from jax.experimental.pallas import tpu as pltpu
from jax.sharding import PartitionSpec as P

BLOCK = 128
MESH = pl.DeviceIdType.MESH


def schedule(rounds):
    bits = sorted(range(1, rounds + 1), key=lambda k: (k.bit_count(), k))
    near = [k for k in bits if k.bit_count() == 1]
    return [k - 1 for k in near[1:2] + near[3:] + near[:1] + bits[len(near) :] + near[2:3]]


def kernel(
    n, reps, pts_hbm, nrm_hbm, src_hbm, tgt_hbm, act_hbm, out,
    pts, nrm, src, tgt, act, stage, inbox, prod, res, got, own, other,
    load, out_send, out_recv, back_send, back_recv, pair_send, pair_recv,
):
    rounds, per_rep = tgt.shape[0], tgt.shape[3]
    npts = pts.shape[1] * BLOCK
    me = lax.axis_index("blk")
    half = lax.axis_index("rep")
    partner = 1 - half
    order = schedule(rounds)

    offsets = sorted({k % n for k in range(1, rounds + 1)} | {-k % n for k in range(1, rounds + 1)})
    barrier = pltpu.get_barrier_semaphore()
    for d in offsets:
        pl.semaphore_signal(
            barrier, inc=1, device_id={"blk": lax.rem(me + d, n), "rep": half}, device_id_type=MESH
        )
    pl.semaphore_signal(barrier, inc=1, device_id={"blk": me, "rep": partner}, device_id_type=MESH)

    pairs = ((src_hbm, src), (act_hbm, act), (tgt_hbm, tgt), (pts_hbm, pts), (nrm_hbm, nrm))
    loads = [pltpu.make_async_copy(a, b, load.at[i]) for i, (a, b) in enumerate(pairs)]
    for copy in loads:
        copy.start()
    prod[...] = jnp.zeros_like(prod)
    res[...] = jnp.zeros_like(res)
    for copy in loads[:4]:
        copy.wait()

    slot = lax.broadcasted_iota(jnp.int32, (per_rep, BLOCK), 0) + half * per_rep
    for k in range(rounds):
        for j in range(per_rep):
            block = src[k, 0, 0, j]
            for c in range(3):
                stage[k, c * per_rep + j, :] = pts[c, block]
        index = jnp.where(slot < act[0, k], tgt[k, 0, 0], npts)
        stage[k, 3 * per_rep :, :] = index.astype(jnp.float32)

    pl.semaphore_wait(barrier, len(offsets) + 1)

    def outgoing(k):
        return pltpu.make_async_remote_copy(
            src_ref=stage.at[k],
            dst_ref=inbox.at[k],
            send_sem=out_send.at[k],
            recv_sem=out_recv.at[k],
            device_id={"blk": lax.rem(me + n - (k + 1), n), "rep": half},
            device_id_type=MESH,
        )

    def returned(k):
        return pltpu.make_async_remote_copy(
            src_ref=res.at[k],
            dst_ref=got.at[k],
            send_sem=back_send.at[k],
            recv_sem=back_recv.at[k],
            device_id={"blk": lax.rem(me + k + 1, n), "rep": half},
            device_id_type=MESH,
        )

    for k in order:
        outgoing(k).start()
    loads[4].wait()

    def terms(k):
        p = [inbox[k, c * per_rep : (c + 1) * per_rep, :] for c in range(3)]
        index = inbox[k, 3 * per_rep :, :].astype(jnp.int32)
        lane = index & (BLOCK - 1)
        row = index >> (BLOCK.bit_length() - 1)
        found = [jnp.zeros((per_rep, BLOCK), jnp.float32) for _ in range(6)]
        for h in range(npts // BLOCK):
            here = row == h
            for c in range(6):
                table = pts if c < 3 else nrm
                line = table[c % 3, h : h + 1, :]
                line = jnp.broadcast_to(line, (per_rep, BLOCK))
                value = jnp.take_along_axis(line, lane, axis=1, mode="promise_in_bounds")
                found[c] = jnp.where(here, value, found[c])
        q, m = found[:3], found[3:]
        resid = m[0] * (p[0] - q[0]) + m[1] * (p[1] - q[1]) + m[2] * (p[2] - q[2])
        weight = 1.0 / (1.0 + resid * resid)
        jacob = [
            p[1] * m[2] - p[2] * m[1],
            p[2] * m[0] - p[0] * m[2],
            p[0] * m[1] - p[1] * m[0],
            m[0],
            m[1],
            m[2],
        ]
        for i in range(6):
            scaled = jacob[i] * weight
            for j in range(i, 6):
                line = jnp.sum(scaled * jacob[j], axis=0, keepdims=True)
                prod[k, 6 * i + j : 6 * i + j + 1, :] = line
                if j != i:
                    prod[k, 6 * j + i : 6 * j + i + 1, :] = line
            prod[k, 36 + i : 37 + i, :] = jnp.sum(scaled * resid, axis=0, keepdims=True)

    width = prod.shape[1]
    ones = jnp.ones((8, BLOCK), jnp.float32)

    def lane_sums(k):
        sums = lax.dot_general(
            ones, prod[k], (((1,), (1,)), ((), ())),
            precision=lax.Precision.HIGHEST, preferred_element_type=jnp.float32,
        )
        res[k, :, :width] = sums[:1] / (reps * per_rep * BLOCK)

    before = None
    for k in order:
        outgoing(k).wait_recv()
        if before is not None:
            lane_sums(before)
        terms(k)
        if before is not None:
            returned(before).start()
        before = k
    lane_sums(before)
    returned(before).start()
    lanes = lax.broadcasted_iota(jnp.int32, (1, BLOCK), 1)
    sign = jnp.where(lanes < 36, 1.0, -1.0)
    total = res[0]
    for k in range(1, rounds):
        total = total + res[k]
    total = total * sign
    for k in order:
        outgoing(k).wait_send()
    for k in order:
        returned(k).wait_recv()
        own[k : k + 1, :] = got[k]
        total = total + got[k]
    own[rounds : rounds + 1, :] = total / (2.0 * rounds)
    swap = pltpu.make_async_remote_copy(
        src_ref=own,
        dst_ref=other,
        send_sem=pair_send,
        recv_sem=pair_recv,
        device_id={"blk": me, "rep": partner},
        device_id_type=MESH,
    )
    swap.start()
    for k in order:
        returned(k).wait_send()
    swap.wait()
    out[...] = own[...] + other[...]


def split(sums, diag_ref, grad_ref, pair_ref):
    rounds = pair_ref.shape[0]
    for k in range(rounds):
        pair_ref[k, 0] = sums[k : k + 1, :36]
    diag_ref[...] = sums[rounds : rounds + 1, :36]
    grad_ref[...] = sums[rounds : rounds + 1, 36:42]


def by_rows(scan):
    return jnp.moveaxis(scan, 1, 0).reshape(scan.shape[1], -1, BLOCK)


def body(n, reps, points, normals, src_block, tgt_index, active):
    rounds, count = src_block.shape[:2]
    per_rep = src_block.shape[3]
    if count != 1 or reps != 2 or rounds >= n:
        raise ValueError("unsupported sizes")
    vmem = pl.BlockSpec(memory_space=pltpu.VMEM)
    f32, i32 = jnp.float32, jnp.int32
    rows = points.shape[2] // BLOCK
    sums = pl.pallas_call(
        functools.partial(kernel, n, reps),
        out_shape=pltpu.VMEM((rounds + 1, BLOCK), f32),
        in_specs=[pl.BlockSpec(memory_space=pl.ANY)] * 5,
        out_specs=vmem,
        scratch_shapes=[
            pltpu.VMEM((3, rows, BLOCK), f32),
            pltpu.VMEM((3, rows, BLOCK), f32),
            pltpu.SMEM(src_block.shape, i32),
            pltpu.VMEM(tgt_index.shape, i32),
            pltpu.SMEM((1, rounds), i32),
            pltpu.VMEM((rounds, 4 * per_rep, BLOCK), f32),
            pltpu.VMEM((rounds, 4 * per_rep, BLOCK), f32),
            pltpu.VMEM((rounds, 48, BLOCK), f32),
            pltpu.VMEM((rounds, 1, BLOCK), f32),
            pltpu.VMEM((rounds, 1, BLOCK), f32),
            pltpu.VMEM((rounds + 1, BLOCK), f32),
            pltpu.VMEM((rounds + 1, BLOCK), f32),
            pltpu.SemaphoreType.DMA((5,)),
            pltpu.SemaphoreType.DMA((rounds,)),
            pltpu.SemaphoreType.DMA((rounds,)),
            pltpu.SemaphoreType.DMA((rounds,)),
            pltpu.SemaphoreType.DMA((rounds,)),
            pltpu.SemaphoreType.DMA,
            pltpu.SemaphoreType.DMA,
        ],
        compiler_params=pltpu.CompilerParams(collective_id=0, has_side_effects=True),
        name="normal_equations",
    )(by_rows(points), by_rows(normals), src_block, tgt_index, active.reshape(1, rounds))
    return pl.pallas_call(
        split,
        out_shape=(
            jax.ShapeDtypeStruct((1, 36), f32),
            jax.ShapeDtypeStruct((1, 6), f32),
            jax.ShapeDtypeStruct((rounds, 1, 1, 36), f32),
        ),
        in_specs=[vmem],
        out_specs=(vmem, vmem, vmem),
        name="split_sums",
    )(pltpu.with_memory_space_constraint(sums, pltpu.VMEM))


def solution(mesh):
    return jax.shard_map(
        functools.partial(body, mesh.shape["blk"], mesh.shape["rep"]),
        mesh=mesh,
        in_specs=(
            P("blk", None, None),
            P("blk", None, None),
            P(None, "blk", None, "rep"),
            P(None, "blk", None, "rep", None),
            P(None, "blk", None),
        ),
        out_specs=(P("blk", None), P("blk", None), P(None, "blk", None, None)),
        check_vma=False,
    )
```
